128 devices in a mesh: dp: 16 (over x, z), expert: 8 (over y, core).
Axes of the slice: x: 4, y: 4, z: 4, core: 2. Of those that a mesh axis runs over, the one named last changes fastest.
Arguments:
- tokens: bfloat16 [16384, 2048], P(('dp', 'expert')), may hold values from -6 to 6
- out_grad: bfloat16 [16384, 2048], P(('dp', 'expert')), may hold values from -3 to 3
- z_weight: float32 [16384], P(('dp', 'expert')), may hold values from 0.1 to 1
- router_weight: bfloat16 [2048, 128], replicated, may hold values from -0.125 to 0.125
- expert_ids: int32 [16384, 4], P(('dp', 'expert')), may hold values from 0 to 127, as said below
- gate_up_weight: bfloat16 [8, 2048, 3072], P('expert'), may hold values from -0.125 to 0.125
- down_weight: bfloat16 [8, 1536, 2048], P('expert'), may hold values from -0.15625 to 0.15625
Outputs:
- token_grad: bfloat16 [16384, 2048], P(('dp', 'expert'))
- router_grad: float32 [2048, 128], replicated
- gate_up_grad: bfloat16 [8, 2048, 3072], P('expert', 'dp')
- down_grad: bfloat16 [8, 1536, 2048], P('expert', 'dp')
The draws below stay inside these ranges and needn't reach their ends.
Inputs may be any that keep to these rules, and one draw needn't show every extreme that they name: `expert_ids`: each row names 4 different experts. Experts 0 to 7 are the ones in flight. The 128 rows of one device name any one expert in flight at most 64 times; in every data group some expert in flight is named exactly 64 times by the rows of each device of the group.
All inputs are finite; a program needn't handle non-finite values.
Results may differ from the reference program's by a relative error of at most 0.019.
Values may be sent and summed in bfloat16 or wider, within the bound.
No kernel may reach another device: no remote copies, remote signals or barrier semaphores. Data moves between devices by JAX's collectives and lax.ppermute only.
A program may use at most 192 MiB of HBM per device.

```python
import math
import jax
import jax.numpy as jnp
from jax import lax

D = 2048
FF = 1536
ROUTED = 128
TOP = 4
BLOCK = 128
TOK_DEV = 128
CAP = 64
FLIGHT = 8
TOKENS = 16384
N_DP = 16
N_EXPERT = 8


def draw_expert_ids(key, part):
    devices_all = TOKENS // TOK_DEV
    flight = N_EXPERT
    key_base, key_mask, key_hot, key_dev = jax.random.split(key, 4)
    base = jax.random.randint(key_base, (devices_all, flight), 0, CAP + 1)
    base = base * jax.random.randint(key_mask, (devices_all, flight), 0, 2)
    hot = jax.random.randint(key_hot, (devices_all // N_EXPERT,), 0, flight)
    hot_dev = jnp.repeat(hot, N_EXPERT)
    counts = jnp.where(jnp.arange(flight)[None, :] == hot_dev[:, None], CAP, base).astype(jnp.int32)
    others = ROUTED - flight
    spacing = others // TOP

    def one_device(count_row, dev_key):
        key_fill, key_order, key_perm = jax.random.split(dev_key, 3)
        ends = jnp.cumsum(count_row)
        total = ends[-1]
        demand = jnp.arange(TOP * TOK_DEV, dtype=jnp.int32)
        owner = jnp.sum((ends[None, :] <= demand[:, None]).astype(jnp.int32), axis=1)
        table = jnp.where(demand < total, owner, -1).reshape(TOP, TOK_DEV).T
        offset = jax.random.randint(key_fill, (TOK_DEV, 1), 0, others)
        fill = flight + (offset + jnp.arange(TOP, dtype=jnp.int32)[None, :] * spacing) % others
        table = jnp.where(table >= 0, table, fill)
        order_keys = jax.random.randint(key_order, (TOK_DEV, TOP), 0, 1 << 20) * TOP + jnp.arange(TOP, dtype=jnp.int32)[None, :]
        order = jnp.argsort(order_keys, axis=1, stable=True)
        table = jnp.take_along_axis(table, order, axis=1)
        shuffle = jax.random.permutation(key_perm, TOK_DEV)
        return table[shuffle]
    dev_keys = jax.random.split(key_dev, devices_all)
    result = jax.vmap(one_device)(counts, dev_keys)
    return result.reshape(TOKENS, TOP).astype(jnp.int32)


def block_levels(rng, dims, cuts, smallest, high):
    level = 1.0
    for position, shards_of in cuts:
        heights = jax.random.uniform(jax.random.fold_in(jax.random.fold_in(rng, 6), position), (shards_of,), jnp.float32, smallest / len(cuts), high / len(cuts))
        level = level * jnp.repeat(jnp.exp(heights), dims[position] // shards_of).reshape((-1,) + (1,) * (len(dims) - 1 - position))
    return level


def normal_values(rng, extent, scale, limit, shards=(), kind=jnp.bfloat16):
    entries = scale * jax.random.normal(rng, extent, jnp.float32)
    if shards:
        entries = entries * block_levels(rng, extent, shards, -0.22, 0.18)
    return jnp.clip(entries, -limit, limit).astype(kind)


def setup_inputs(seed: int = 0) -> dict:
    key_list = jax.random.split(jax.random.key(seed), 8)
    tokens = normal_values(key_list[0], (TOKENS, D), 1.0, 6.0, ((0, 128),))
    out_grad = normal_values(key_list[1], (TOKENS, D), 0.5, 3.0, ((0, 128),))
    z_weight = jnp.clip(jnp.exp(math.log(1.0) - 2.3025851 * jax.random.uniform(key_list[2], (TOKENS,), jnp.float32) ** block_levels(key_list[2], (TOKENS,), ((0, 128),), -0.2, 0.2)), 0.1, 1.0)
    router_weight = normal_values(key_list[3], (D, ROUTED), D ** -0.5, 0.125)
    expert_ids = draw_expert_ids(jax.random.fold_in(key_list[7], 71), 0)
    gate_up_weight = normal_values(key_list[5], (FLIGHT, D, 2 * FF), D ** -0.5, 0.125, ((0, 8),))
    down_weight = normal_values(key_list[6], (FLIGHT, FF, D), FF ** -0.5, 0.15625, ((0, 8),))
    return dict(tokens=tokens, out_grad=out_grad, z_weight=z_weight, router_weight=router_weight, expert_ids=expert_ids, gate_up_weight=gate_up_weight, down_weight=down_weight)


def expert_rows(rows_in, rows_grad, w_gateup, w_down, acc_gateup, acc_down):
    hidden_units = w_down.shape[0]
    pre_act = jnp.dot(rows_in, w_gateup, preferred_element_type=jnp.float32)
    gate_pre = pre_act[:, :hidden_units]
    up_pre = pre_act[:, hidden_units:]
    activated = jax.nn.silu(gate_pre)
    hidden = (activated * up_pre).astype(jnp.bfloat16)
    expert_out = jnp.dot(hidden, w_down, preferred_element_type=jnp.float32).astype(jnp.bfloat16)
    hidden_grad = lax.dot_general(rows_grad, w_down, (((1,), (1,)), ((), ())), preferred_element_type=jnp.float32)
    acc_down = acc_down + lax.dot_general(hidden, rows_grad, (((0,), (0,)), ((), ())), preferred_element_type=jnp.float32)
    sigmoid_gate = jax.nn.sigmoid(gate_pre)
    gate_grad = hidden_grad * up_pre * sigmoid_gate * (1.0 + gate_pre * (1.0 - sigmoid_gate))
    up_grad = hidden_grad * activated
    pre_grad = jnp.concatenate([gate_grad, up_grad], axis=1).astype(jnp.bfloat16)
    acc_gateup = acc_gateup + lax.dot_general(rows_in, pre_grad, (((0,), (0,)), ((), ())), preferred_element_type=jnp.float32)
    input_grad = lax.dot_general(pre_grad, w_gateup, (((1,), (1,)), ((), ())), preferred_element_type=jnp.float32).astype(jnp.bfloat16)
    return acc_gateup, acc_down, expert_out, input_grad


def run_blocks(work_in, work_grad, w_gateup, w_down, nblocks):
    width = work_in.shape[1]
    hidden_units = w_down.shape[0]
    start_state = (jnp.zeros((width, 2 * hidden_units), jnp.float32), jnp.zeros((hidden_units, width), jnp.float32),
                   jnp.zeros_like(work_in), jnp.zeros_like(work_in))

    def step(block_index, carry):
        acc_gateup, acc_down, out_rows, grad_rows = carry
        start = (block_index * BLOCK).astype(jnp.int32)
        rows_in = lax.dynamic_slice_in_dim(work_in, start, BLOCK, 0)
        rows_grad = lax.dynamic_slice_in_dim(work_grad, start, BLOCK, 0)
        acc_gateup, acc_down, produced, backward = expert_rows(rows_in, rows_grad, w_gateup, w_down, acc_gateup, acc_down)
        out_rows = lax.dynamic_update_slice_in_dim(out_rows, produced, start, 0)
        grad_rows = lax.dynamic_update_slice_in_dim(grad_rows, backward, start, 0)
        return acc_gateup, acc_down, out_rows, grad_rows

    return lax.fori_loop(jnp.int32(0), nblocks.astype(jnp.int32), step, start_state)


def reference(tokens, out_grad, z_weight, router_weight, expert_ids, gate_up_weight, down_weight):
    logits = jnp.dot(tokens, router_weight, preferred_element_type=jnp.float32)
    choose = expert_ids[:, :, None] == jnp.arange(ROUTED, dtype=jnp.int32)[None, None, :]
    selected = jnp.sum(jnp.where(choose, logits[:, None, :], 0.0), axis=2)
    sel_exp = jnp.exp(selected)
    probs = sel_exp / jnp.sum(sel_exp, axis=1, keepdims=True)
    log_total = jnp.log(jnp.sum(jnp.exp(logits), axis=1))
    slots_group = N_EXPERT * TOK_DEV * TOP
    rows_max = N_EXPERT * CAP
    group_ids = expert_ids.reshape(N_DP, slots_group)
    group_prob = probs.reshape(N_DP, slots_group)
    group_tok = tokens.reshape(N_DP, N_EXPERT * TOK_DEV, D)
    group_grad = out_grad.reshape(N_DP, N_EXPERT * TOK_DEV, D)

    def one_group(carry, data):
        ids_here, prob_here, tok_here, grad_here = data

        def one_expert(expert):
            member = ids_here == expert
            rank = jnp.cumsum(member.astype(jnp.int32)) - 1
            place = jnp.where(member, rank, rows_max).astype(jnp.int32)
            source = jnp.zeros((rows_max,), jnp.int32).at[place].set(jnp.arange(slots_group, dtype=jnp.int32), mode="drop")
            valid = jnp.zeros((rows_max,), jnp.bool_).at[place].set(True, mode="drop")
            tok_index = source // TOP
            rows_in = jnp.where(valid[:, None], tok_here[tok_index], 0)
            rows_grad = jnp.where(valid[:, None], prob_here[source][:, None] * grad_here[tok_index].astype(jnp.float32), 0.0).astype(jnp.bfloat16)
            used = (jnp.sum(member.astype(jnp.int32)) + BLOCK - 1) // BLOCK
            acc_gateup, acc_down, produced, backward = run_blocks(rows_in, rows_grad, gate_up_weight[expert], down_weight[expert], used)
            return acc_gateup.astype(jnp.bfloat16), acc_down.astype(jnp.bfloat16), produced, backward, source, valid

        part_gu, part_down, outs, backs, sources, valids = lax.map(one_expert, jnp.arange(N_EXPERT, dtype=jnp.int32))
        sum_gu, sum_down = carry
        sum_gu = sum_gu + part_gu.astype(jnp.float32)
        sum_down = sum_down + part_down.astype(jnp.float32)
        target = jnp.where(valids.reshape(-1), sources.reshape(-1), slots_group).astype(jnp.int32)
        slot_out = jnp.zeros((slots_group, D), jnp.bfloat16).at[target].set(outs.reshape(-1, D), mode="drop")
        slot_back = jnp.zeros((slots_group, D), jnp.bfloat16).at[target].set(backs.reshape(-1, D), mode="drop")
        return (sum_gu, sum_down), (slot_out, slot_back)

    start_sums = (jnp.zeros((N_EXPERT, D, 2 * FF), jnp.float32), jnp.zeros((N_EXPERT, FF, D), jnp.float32))
    (sum_gu, sum_down), (slot_out, slot_back) = lax.scan(one_group, start_sums, (group_ids, group_prob, group_tok, group_grad))
    slot_out = slot_out.reshape(TOKENS, TOP, D)
    slot_back = slot_back.reshape(TOKENS, TOP, D)
    scores = jnp.sum(out_grad[:, None, :].astype(jnp.float32) * slot_out.astype(jnp.float32), axis=2)
    mean_score = jnp.sum(probs * scores, axis=1, keepdims=True)
    sel_grad = probs * (scores - mean_score)
    z_grad = 2.0 * z_weight[:, None] * log_total[:, None] * jnp.exp(logits - log_total[:, None])
    logit_grad = (z_grad + jnp.sum(jnp.where(choose, sel_grad[:, :, None], 0.0), axis=1)).astype(jnp.bfloat16)
    token_grad = (jnp.sum(slot_back.astype(jnp.float32), axis=1)
                  + lax.dot_general(logit_grad, router_weight, (((1,), (1,)), ((), ())), preferred_element_type=jnp.float32)).astype(jnp.bfloat16)
    router_grad = lax.dot_general(tokens, logit_grad, (((0,), (0,)), ((), ())), preferred_element_type=jnp.float32)
    return token_grad, router_grad, sum_gu.astype(jnp.bfloat16), sum_down.astype(jnp.bfloat16)
```

```python
import jax
import jax.numpy as jnp
from jax import lax
from jax.sharding import Mesh, PartitionSpec as P


BF = jnp.bfloat16
F32 = jnp.float32
OFFSETS = [(0, 0), (0, 1), (1, 0), (1, 1), (-1, 0), (-1, 1), (2, 0), (2, 1)]


def shift(a, axis, step):
    n = lax.axis_size(axis)
    return lax.ppermute(a, axis, [(i, (i + step) % n) for i in range(n)])


def hop(a, dy, cc):
    if dy == 0 and cc == 0:
        return a
    ny = lax.axis_size("y")
    perm = []
    for y in range(ny):
        for c in range(2):
            perm.append((y * 2 + c, ((y + dy) % ny) * 2 + (c ^ cc)))
    return lax.ppermute(a, ("y", "c"), perm)


def swap(a):
    return lax.ppermute(a, "c", [(0, 1), (1, 0)])


def gather_group(a):
    half = a.shape[0] // 2
    left = shift(a, "y", 1)
    right = shift(a, "y", -1)
    far = jnp.concatenate([shift(left[:half], "y", 1), shift(right[half:], "y", -1)], axis=0)
    pieces = []
    for part in (a, left, right, far):
        pieces += [part, swap(part)]
    return pieces


def pick(blocks, index, axis):
    return lax.dynamic_index_in_dim(blocks, index, axis, keepdims=False)


def ring_sum(blocks, dim, axis):
    me = lax.axis_index(axis)
    b0, b1, b2, b3 = (pick(blocks, (me + k) % 4, dim) for k in range(4))
    h = b0.shape[-1] // 2
    a_up = shift(b2[..., :h], axis, 1)
    a_dn = shift(b2[..., h:], axis, -1)
    b_up = shift(b1[..., h:], axis, 1)
    b_dn = shift(b3[..., :h], axis, -1)
    c_up = shift((b1[..., :h].astype(F32) + a_up.astype(F32)).astype(BF), axis, 1)
    c_dn = shift((b3[..., h:].astype(F32) + a_dn.astype(F32)).astype(BF), axis, -1)
    lo = b0[..., :h].astype(F32) + c_up.astype(F32) + b_dn.astype(F32)
    hi = b0[..., h:].astype(F32) + b_up.astype(F32) + c_dn.astype(F32)
    return jnp.concatenate([lo, hi], axis=-1).astype(BF)


def grid_sum(first, second):
    p = ring_sum(first, 0, "x")
    q = ring_sum(second, 1, "z")
    return jnp.concatenate([ring_sum(p, 0, "z"), ring_sum(q, 0, "x")], axis=-1)


def tdot(a, b):
    return lax.dot_general(a, b, (((0,), (0,)), ((), ())), preferred_element_type=F32)


def dot_t(a, b):
    return lax.dot_general(a, b, (((1,), (1,)), ((), ())), preferred_element_type=F32)


def per_device(tokens, out_grad, z_weight, router_weight, expert_ids, gate_up_weight, down_weight):
    tok, width = tokens.shape
    routed = router_weight.shape[1]
    cap = tok // 2
    w_gu = gate_up_weight[0]
    w_dn = down_weight[0]
    ff = w_dn.shape[0]
    my_y = lax.axis_index("y")
    my_c = lax.axis_index("c")
    x_parts = gather_group(tokens)
    g_parts = gather_group(out_grad)

    logits = jnp.dot(tokens, router_weight, preferred_element_type=F32)
    names = jnp.arange(routed, dtype=jnp.int32)[None, :]
    chosen = expert_ids[:, 0:1] == names
    for k in range(1, expert_ids.shape[1]):
        chosen = chosen | (expert_ids[:, k : k + 1] == names)
    expl = jnp.exp(logits)
    sel_exp = jnp.where(chosen, expl, 0.0)
    probs = sel_exp / jnp.sum(sel_exp, axis=1, keepdims=True)
    log_total = jnp.log(jnp.sum(expl, axis=1, keepdims=True))
    experts = jnp.stack([((my_y + dy) % 4) * 2 + (my_c ^ cc) for dy, cc in OFFSETS]).astype(jnp.int32)
    mine = names == experts[:, None]
    member = jnp.max(jnp.where(mine[:, None, :] & chosen[None], 1.0, 0.0), axis=2)
    prob_of = jnp.sum(jnp.where(mine[:, None, :], probs[None], 0.0), axis=2)
    before = (jnp.arange(tok)[:, None] < jnp.arange(tok)[None, :]).astype(BF)
    rank = jnp.dot(member.astype(BF), before, preferred_element_type=F32)
    code = jnp.where(member > 0.0, rank, -1.0)
    msg = jnp.stack([code, prob_of], axis=1)
    got = jnp.stack([hop(msg[j], *OFFSETS[j]) for j in range(8)])
    slots = jnp.arange(cap, dtype=F32)[None, :, None]
    take = got[:, 0, None, :] == slots
    row_prob = jnp.sum(jnp.where(take, got[:, 1, None, :], 0.0), axis=2).reshape(8 * cap, 1)
    take = take.astype(BF)

    def compact(parts):
        rows = [jnp.dot(take[j], parts[j], preferred_element_type=F32).astype(BF) for j in range(8)]
        return jnp.concatenate(rows, axis=0)

    x = compact(x_parts)
    pre_act = jnp.dot(x, w_gu, preferred_element_type=F32)
    gate = pre_act[:, :ff]
    up = pre_act[:, ff:]
    sig = jax.nn.sigmoid(gate)
    silu = gate * sig
    hidden = (silu * up).astype(BF)
    dy = compact(g_parts)
    dyk = (row_prob * dy.astype(F32)).astype(BF)
    part_dn = tdot(hidden, dyk).astype(BF)
    raw = dot_t(dy, w_dn)
    score = jnp.sum(hidden.astype(F32) * raw, axis=1)
    h_grad = row_prob * raw
    pre_gate = (h_grad * up * sig * (1.0 + gate * (1.0 - sig))).astype(BF)
    pre_up = (h_grad * silu).astype(BF)
    part_gate = tdot(x, pre_gate).astype(BF)
    part_up = tdot(x, pre_up).astype(BF)

    half = width // 2
    dn4 = part_dn.reshape(4, 4, ff // 16, width)
    down_grad = grid_sum(dn4[..., :half], dn4[..., half:])
    gate_up_grad = grid_sum(
        part_gate.reshape(4, 4, width // 16, ff), part_up.reshape(4, 4, width // 16, ff)
    )

    score = score.reshape(8, 1, cap)
    home_score = jnp.stack([hop(score[j], -OFFSETS[j][0], OFFSETS[j][1]) for j in range(8)])
    row_grad = (dot_t(pre_gate, w_gu[:, :ff]) + dot_t(pre_up, w_gu[:, ff:])).astype(BF)
    row_grad = row_grad.reshape(8, cap, width)
    home_rows = jnp.concatenate([hop(row_grad[j], -OFFSETS[j][0], OFFSETS[j][1]) for j in range(8)])

    back = (code[:, None, :] == slots)
    score_of = jnp.sum(jnp.where(back, home_score.reshape(8, cap, 1), 0.0), axis=1)
    scores = jnp.sum(jnp.where(mine[:, None, :], score_of[:, :, None], 0.0), axis=0)
    scores = jnp.where(chosen, scores, 0.0)
    mean_score = jnp.sum(probs * scores, axis=1, keepdims=True)
    z_grad = 2.0 * z_weight[:, None] * log_total * jnp.exp(logits - log_total)
    logit_grad = (z_grad + probs * (scores - mean_score)).astype(BF)
    router_part = tdot(tokens, logit_grad)
    router_grad = lax.psum(router_part, ("x", "z", "y", "c"))
    token_grad = (
        tdot(back.astype(BF).reshape(8 * cap, tok), home_rows) + dot_t(logit_grad, router_weight)
    ).astype(BF)
    return token_grad, router_grad, gate_up_grad[None], down_grad[None]


def solution(mesh):
    grid = Mesh(mesh.devices.reshape(4, 4, 4, 2), ("x", "z", "y", "c"))
    every = ("x", "z", "y", "c")
    return jax.shard_map(
        per_device,
        mesh=grid,
        in_specs=(
            P(every, None),
            P(every, None),
            P(every),
            P(),
            P(every, None),
            P(("y", "c"), None, None),
            P(("y", "c"), None, None),
        ),
        out_specs=(
            P(every, None),
            P(),
            P(("y", "c"), ("x", "z"), None),
            P(("y", "c"), ("x", "z"), None),
        ),
        check_vma=False,
    )
```

```python
import jax
import jax.numpy as jnp
from jax import lax
from jax.sharding import Mesh, PartitionSpec as P


BF = jnp.bfloat16
F32 = jnp.float32
DP = ("x", "z")
GROUP = ("y", "c")


def shift(a, step):
    return lax.ppermute(a, "y", [(i, (i + step) % 4) for i in range(4)])


def swap(a):
    return lax.ppermute(a, "c", [(0, 1), (1, 0)])


def spread(left, right):
    half = left.shape[0] // 2
    return jnp.concatenate([shift(left[:half], 1), shift(right[half:], -1)], axis=0)


def tdot(a, b):
    return lax.dot_general(a, b, (((0,), (0,)), ((), ())), preferred_element_type=F32)


def dot_t(a, b):
    return lax.dot_general(a, b, (((1,), (1,)), ((), ())), preferred_element_type=F32)


def send_each(a):
    return lax.all_to_all(a, GROUP, split_axis=0, concat_axis=0, tiled=True)


def sum_all(a):
    step = a.shape[0] // 128
    pieces = tuple(a[k * step : (k + 1) * step] for k in range(128))
    return jnp.concatenate(lax.psum(pieces, ("x", "z", "y", "c")), axis=0)


def per_device(tokens, out_grad, z_weight, router_weight, expert_ids, gate_up_weight, down_weight):
    tok, width = tokens.shape
    routed = router_weight.shape[1]
    cap = tok // 2
    w_gu = gate_up_weight[0]
    w_dn = down_weight[0]
    ff = w_dn.shape[0]
    my_y = lax.axis_index("y")
    my_c = lax.axis_index("c")

    x1, x3 = shift(tokens, 1), shift(tokens, -1)
    x2 = spread(x1, x3)
    later, x1, x3 = lax.optimization_barrier((out_grad, x1, x3))
    g1, g3 = shift(later, 1), shift(later, -1)
    g2 = spread(g1, g3)
    x_parts, g_parts = [], []
    for part in (tokens, x1, x2, x3):
        x_parts += [part, swap(part)]
    for part in (out_grad, g1, g2, g3):
        g_parts += [part, swap(part)]
    origin = [((my_y - k) % 4) * 2 + (my_c ^ cc) for k in range(4) for cc in range(2)]
    place = [((my_y - s // 2) % 4) * 2 + (my_c ^ (s % 2)) for s in range(8)]

    logits = jnp.dot(tokens, router_weight, preferred_element_type=F32)
    names = jnp.arange(routed, dtype=jnp.int32)[None, :]
    chosen = expert_ids[:, 0:1] == names
    for k in range(1, expert_ids.shape[1]):
        chosen = chosen | (expert_ids[:, k : k + 1] == names)
    expl = jnp.exp(logits)
    sel_exp = jnp.where(chosen, expl, 0.0)
    probs = jnp.where(chosen, sel_exp / jnp.sum(sel_exp, axis=1, keepdims=True), 0.0)
    log_total = jnp.log(jnp.sum(expl, axis=1, keepdims=True))
    member = jnp.where(chosen[:, :8], 1.0, 0.0).T
    before = (jnp.arange(tok)[:, None] < jnp.arange(tok)[None, :]).astype(BF)
    rank = jnp.dot(member.astype(BF), before, preferred_element_type=F32)
    code = jnp.where(member > 0.0, rank, -1.0)
    got = send_each(jnp.stack([code, probs[:, :8].T], axis=1))
    got = jnp.concatenate([lax.dynamic_slice_in_dim(got, s, 1, 0) for s in origin], axis=0)
    slots = jnp.arange(cap, dtype=F32)[None, :, None]
    take = got[:, 0, None, :] == slots
    row_prob = jnp.sum(jnp.where(take, got[:, 1, None, :], 0.0), axis=2).reshape(8 * cap, 1)
    take = take.astype(BF)

    def compact(parts):
        rows = [jnp.dot(take[j], parts[j], preferred_element_type=F32).astype(BF) for j in range(8)]
        return jnp.concatenate(rows, axis=0)

    x = compact(x_parts)
    pre_act = jnp.dot(x, w_gu, preferred_element_type=F32)
    gate = pre_act[:, :ff]
    up = pre_act[:, ff:]
    sig = jax.nn.sigmoid(gate)
    silu = gate * sig
    hidden = (silu * up).astype(BF)
    dy = compact(g_parts)
    dyk = (row_prob * dy.astype(F32)).astype(BF)
    raw = dot_t(dy, w_dn)
    score = jnp.sum(hidden.astype(F32) * raw, axis=1)
    h_grad = row_prob * raw
    pre_gate = (h_grad * up * sig * (1.0 + gate * (1.0 - sig))).astype(BF)
    pre_up = (h_grad * silu).astype(BF)

    cols = ff // 3
    parts = []
    for b in (pre_gate, pre_up):
        for q in range(3):
            g = tdot(x, b[:, q * cols : (q + 1) * cols]).astype(BF)
            parts.append(g.reshape(16, width // 16, cols))
    for q in range(width // cols):
        g = tdot(hidden, dyk[:, q * cols : (q + 1) * cols]).astype(BF)
        parts.append(g.reshape(16, ff // 16, cols))
    parts = jnp.concatenate(parts, axis=1).reshape(1, -1, cols)
    total = lax.psum_scatter(parts, DP, scatter_dimension=1, tiled=True)[0]
    r = width // 16
    gate_up_grad = jnp.concatenate([total[q * r : (q + 1) * r] for q in range(6)], axis=1)
    rest = total[6 * r :]
    r = ff // 16
    down_grad = jnp.concatenate([rest[q * r : (q + 1) * r] for q in range(width // cols)], axis=1)

    home_score = send_each(jnp.concatenate(
        [lax.dynamic_slice_in_dim(score.reshape(8, 1, cap), s, 1, 0) for s in place], axis=0))
    row_grad = (dot_t(pre_gate, w_gu[:, :ff]) + dot_t(pre_up, w_gu[:, ff:])).astype(BF)
    row_grad = row_grad.reshape(8, cap, width)
    home_rows = send_each(jnp.concatenate(
        [lax.dynamic_slice_in_dim(row_grad, s, 1, 0) for s in place], axis=0))

    back = code[:, None, :] == slots
    score_of = jnp.sum(jnp.where(back, home_score.reshape(8, cap, 1), 0.0), axis=1)
    scores = jnp.concatenate([score_of.T, jnp.zeros((tok, routed - 8), F32)], axis=1)
    mean_score = jnp.sum(probs * scores, axis=1, keepdims=True)
    z_grad = 2.0 * z_weight[:, None] * log_total * jnp.exp(logits - log_total)
    logit_grad = (z_grad + probs * (scores - mean_score)).astype(BF)
    router_grad = sum_all(tdot(tokens, logit_grad))
    token_grad = (
        tdot(back.astype(BF).reshape(8 * cap, tok), home_rows.reshape(8 * cap, width))
        + dot_t(logit_grad, router_weight)
    ).astype(BF)
    return token_grad, router_grad, gate_up_grad[None], down_grad[None]


def solution(mesh):
    grid = Mesh(mesh.devices.reshape(4, 4, 4, 2), ("x", "z", "y", "c"))
    every = ("x", "z", "y", "c")
    return jax.shard_map(
        per_device,
        mesh=grid,
        in_specs=(
            P(every, None),
            P(every, None),
            P(every),
            P(),
            P(every, None),
            P(GROUP, None, None),
            P(GROUP, None, None),
        ),
        out_specs=(
            P(every, None),
            P(),
            P(GROUP, DP, None),
            P(GROUP, DP, None),
        ),
        check_vma=False,
    )
```

```python
import functools

import jax
import jax.numpy as jnp
from jax import lax
from jax.experimental import pallas as pl
from jax.experimental.pallas import tpu as pltpu
from jax.sharding import Mesh, PartitionSpec as P


BF = jnp.bfloat16
F32 = jnp.float32
DP = ("x", "z")
GROUP = ("y", "c")


def shift(a, step):
    return lax.ppermute(a, "y", [(i, (i + step) % 4) for i in range(4)])


def swap(a):
    return lax.ppermute(a, "c", [(0, 1), (1, 0)])


def spread(left, right):
    half = left.shape[0] // 2
    return jnp.concatenate([shift(left[:half], 1), shift(right[half:], -1)], axis=0)


def tdot(a, b):
    return lax.dot_general(a, b, (((0,), (0,)), ((), ())), preferred_element_type=F32)


def dot_t(a, b):
    return lax.dot_general(a, b, (((1,), (1,)), ((), ())), preferred_element_type=F32)


def send_each(a):
    return lax.all_to_all(a, GROUP, split_axis=0, concat_axis=0, tiled=True)


def ring_all(a, axis):
    others = [lax.ppermute(a, axis, [(i, (i + k) % 4) for i in range(4)]) for k in (1, 2, 3)]
    return a + others[0] + others[1] + others[2]


def grad_kernel(tiles, gate_ref, up_ref, w_ref, x_ref, dy_ref, prob_ref, parts_ref, pre_ref, score_ref, hid, dyk):
    i = pl.program_id(0)
    ff = hid.shape[1]
    tile = gate_ref.shape[1]
    cols = parts_ref.shape[2]

    @pl.when(i == 0)
    def _():
        score_ref[...] = jnp.zeros_like(score_ref)
        dyk[...] = (prob_ref[...] * dy_ref[...].astype(F32)).astype(BF)

    @pl.when(i < tiles)
    def _():
        at = pl.multiple_of(i * tile, tile)
        raw = lax.dot_general(dy_ref[...], w_ref[...], (((1,), (1,)), ((), ())), preferred_element_type=F32)
        gate = gate_ref[...]
        up = up_ref[...]
        sig = 1.0 / (1.0 + jnp.exp(-gate))
        silu = gate * sig
        hidden = (silu * up).astype(BF)
        score_ref[...] += jnp.sum(hidden.astype(F32) * raw, axis=1, keepdims=True)
        grad = prob_ref[...] * raw
        hid[:, pl.ds(at, tile)] = hidden
        pre_ref[:, pl.ds(at, tile)] = (grad * up * sig * (1.0 + gate * (1.0 - sig))).astype(BF)
        pre_ref[:, pl.ds(pl.multiple_of(ff + at, tile), tile)] = (grad * silu).astype(BF)

    @pl.when(i >= tiles)
    def _():
        k = i - tiles
        r = x_ref.shape[1] // 16
        xs = x_ref[:, pl.ds(pl.multiple_of(k * 4 * r, 4 * r), 4 * r)]
        for q in range(2 * ff // cols):
            g = tdot(xs, pre_ref[:, q * cols : (q + 1) * cols]).astype(BF)
            for d in range(4):
                parts_ref[d, q * r : (q + 1) * r, :] = g[d * r : (d + 1) * r]
        base = 2 * ff // cols * r
        r = ff // 16
        hs = hid[:, pl.ds(pl.multiple_of(k * 4 * r, 4 * r), 4 * r)]
        for q in range(dyk.shape[1] // cols):
            g = tdot(hs, dyk[:, q * cols : (q + 1) * cols]).astype(BF)
            for d in range(4):
                parts_ref[d, base + q * r : base + (q + 1) * r, :] = g[d * r : (d + 1) * r]


def weight_grads(pre_act, w_dn, x, dy, row_prob):
    rows, width = x.shape
    ff = w_dn.shape[0]
    tiles = 6
    tile = ff // tiles
    cols = ff // 3
    depth = (2 * ff * (width // 16) + width * (ff // 16)) // cols
    last = tiles - 1
    whole = lambda i: (0, 0)
    return pl.pallas_call(
        functools.partial(grad_kernel, tiles),
        grid=(tiles + 4,),
        in_specs=[
            pl.BlockSpec((rows, tile), lambda i: (0, jnp.minimum(i, last))),
            pl.BlockSpec((rows, tile), lambda i: (0, tiles + jnp.minimum(i, last))),
            pl.BlockSpec((tile, width), lambda i: (jnp.minimum(i, last), 0)),
            pl.BlockSpec((rows, width), whole),
            pl.BlockSpec((rows, width), whole),
            pl.BlockSpec((rows, 1), whole),
        ],
        out_specs=[
            pl.BlockSpec((4, depth, cols), lambda i: (jnp.maximum(i - tiles, 0), 0, 0)),
            pl.BlockSpec((rows, 2 * ff), whole),
            pl.BlockSpec((rows, 1), whole),
        ],
        out_shape=[
            jax.ShapeDtypeStruct((16, depth, cols), BF),
            jax.ShapeDtypeStruct((rows, 2 * ff), BF),
            jax.ShapeDtypeStruct((rows, 1), F32),
        ],
        scratch_shapes=[pltpu.VMEM((rows, ff), BF), pltpu.VMEM((rows, width), BF)],
        compiler_params=pltpu.CompilerParams(vmem_limit_bytes=34 * 2**20),
        cost_estimate=pl.CostEstimate(
            flops=2 * rows * width * ff * 4, bytes_accessed=36 * 2**20, transcendentals=rows * ff
        ),
        name="weight_grads",
    )(pre_act, pre_act, w_dn, x, dy, row_prob)


def unpack_kernel(in_ref, gu_ref, dn_ref):
    cols = in_ref.shape[1]
    r = gu_ref.shape[0]
    n = gu_ref.shape[1] // cols
    for q in range(n):
        gu_ref[:, q * cols : (q + 1) * cols] = in_ref[q * r : (q + 1) * r, :]
    base = n * r
    r = dn_ref.shape[0]
    for q in range(dn_ref.shape[1] // cols):
        dn_ref[:, q * cols : (q + 1) * cols] = in_ref[base + q * r : base + (q + 1) * r, :]


def unpack(total, width, ff):
    return pl.pallas_call(
        unpack_kernel,
        out_shape=[
            jax.ShapeDtypeStruct((width // 16, 2 * ff), BF),
            jax.ShapeDtypeStruct((ff // 16, width), BF),
        ],
        name="unpack",
    )(total)


def per_device(tokens, out_grad, z_weight, router_weight, expert_ids, gate_up_weight, down_weight):
    tok, width = tokens.shape
    routed = router_weight.shape[1]
    cap = tok // 2
    w_gu = gate_up_weight[0]
    w_dn = down_weight[0]
    ff = w_dn.shape[0]
    my_y = lax.axis_index("y")
    my_c = lax.axis_index("c")

    names = jnp.arange(routed, dtype=jnp.int32)[None, :]
    slots = jnp.arange(cap, dtype=F32)[None, :, None]
    before = (jnp.arange(tok)[:, None] < jnp.arange(tok)[None, :]).astype(BF)
    top = expert_ids.shape[1]
    id_rows = jnp.pad(expert_ids.T.astype(BF), ((0, 16 - top), (0, width - tok)))
    x0 = jnp.concatenate([tokens, id_rows], axis=0)
    logits = jnp.dot(tokens, router_weight, preferred_element_type=F32)
    chosen = expert_ids[:, 0:1] == names
    for k in range(1, top):
        chosen = chosen | (expert_ids[:, k : k + 1] == names)
    expl = jnp.exp(logits)
    sel_exp = jnp.where(chosen, expl, 0.0)
    probs = jnp.where(chosen, sel_exp / jnp.sum(sel_exp, axis=1, keepdims=True), 0.0)
    log_total = jnp.log(jnp.sum(expl, axis=1, keepdims=True))
    mine = probs[:, :8].T
    high = mine.astype(BF)
    low = (mine - high.astype(F32)).astype(BF)
    prob_rows = jnp.pad(jnp.concatenate([high, low], axis=0), ((0, 0), (0, width - tok)))
    g0 = jnp.concatenate([out_grad, prob_rows], axis=0)

    g0, x0 = lax.optimization_barrier((g0, x0))
    x1, x3 = shift(x0, 1), shift(x0, -1)
    g1, g3 = shift(g0, 1), shift(g0, -1)
    x2 = spread(x1, x3)
    g2 = spread(g1, g3)
    x_parts, g_parts = [], []
    for part in (x0, x1, x2, x3):
        x_parts += [part, swap(part)]
    for part in (g0, g1, g2, g3):
        g_parts += [part, swap(part)]
    place = [((my_y - s // 2) % 4) * 2 + (my_c ^ (s % 2)) for s in range(8)]

    me = my_y * 2 + my_c
    named = jnp.stack([p[tok : tok + top, :tok] for p in x_parts])
    member = jnp.max(jnp.where(named == me.astype(BF), 1.0, 0.0), axis=1)
    rank = jnp.dot(member.astype(BF), before, preferred_element_type=F32)
    take = (rank[:, None, :] == slots) & (member[:, None, :] > 0.0)
    pick = (jnp.arange(16, dtype=jnp.int32) % 8 == me)[None, :, None]
    pairs = jnp.stack([p[tok : tok + 16, :tok] for p in g_parts]).astype(F32)
    prob_of = jnp.sum(jnp.where(pick, pairs, 0.0), axis=1)
    row_prob = jnp.sum(jnp.where(take, prob_of[:, None, :], 0.0), axis=2).reshape(8 * cap, 1)
    take = take.astype(BF)

    def compact(parts):
        rows = [jnp.dot(take[j], parts[j][:tok], preferred_element_type=F32).astype(BF) for j in range(8)]
        return jnp.concatenate(rows, axis=0)

    x = compact(x_parts)
    pre_act = jnp.dot(x, w_gu, preferred_element_type=F32)
    dy = compact(g_parts)
    parts, pre, score = weight_grads(pre_act, w_dn, x, dy, row_prob)
    total = lax.psum_scatter(parts.reshape(1, -1, parts.shape[2]), DP, scatter_dimension=1, tiled=True)[0]
    gate_up_grad, down_grad = unpack(total, width, ff)

    home_score = send_each(jnp.concatenate(
        [lax.dynamic_slice_in_dim(score.reshape(8, 1, cap), s, 1, 0) for s in place], axis=0))
    row_grad = dot_t(pre, w_gu).astype(BF)
    row_grad = row_grad.reshape(8, cap, width)
    home_rows = send_each(jnp.concatenate(
        [lax.dynamic_slice_in_dim(row_grad, s, 1, 0) for s in place], axis=0))

    member = jnp.where(chosen[:, :8], 1.0, 0.0).T
    rank = jnp.dot(member.astype(BF), before, preferred_element_type=F32)
    back = (rank[:, None, :] == slots) & (member[:, None, :] > 0.0)
    score_of = jnp.sum(jnp.where(back, home_score.reshape(8, cap, 1), 0.0), axis=1)
    scores = jnp.concatenate([score_of.T, jnp.zeros((tok, routed - 8), F32)], axis=1)
    mean_score = jnp.sum(probs * scores, axis=1, keepdims=True)
    z_grad = 2.0 * z_weight[:, None] * log_total * jnp.exp(logits - log_total)
    logit_grad = (z_grad + probs * (scores - mean_score)).astype(BF)
    share = send_each(logit_grad.T.reshape(8, routed // 8, tok))
    origin = [((my_y - k) % 4) * 2 + (my_c ^ cc) for k in range(4) for cc in range(2)]
    share = jnp.concatenate([lax.dynamic_slice_in_dim(share, o, 1, 0)[0] for o in origin], axis=1)
    group_tokens = jnp.concatenate([p[:tok] for p in x_parts], axis=0)
    router_part = jnp.dot(share, group_tokens, preferred_element_type=F32)
    router_part = ring_all(ring_all(router_part, "x"), "z")
    near = lax.all_gather(router_part, "y", axis=0, tiled=False)
    away = swap(near)
    both = jnp.stack([jnp.where(my_c == 0, near, away), jnp.where(my_c == 0, away, near)], axis=1)
    router_grad = both.reshape(routed, width).T
    token_grad = (
        tdot(back.astype(BF).reshape(8 * cap, tok), home_rows.reshape(8 * cap, width))
        + dot_t(logit_grad, router_weight)
    ).astype(BF)
    return token_grad, router_grad, gate_up_grad[None], down_grad[None]


def solution(mesh):
    grid = Mesh(mesh.devices.reshape(4, 4, 4, 2), ("x", "z", "y", "c"))
    every = ("x", "z", "y", "c")
    return jax.shard_map(
        per_device,
        mesh=grid,
        in_specs=(
            P(every, None),
            P(every, None),
            P(every),
            P(),
            P(every, None),
            P(GROUP, None, None),
            P(GROUP, None, None),
        ),
        out_specs=(
            P(every, None),
            P(),
            P(GROUP, DP, None),
            P(GROUP, DP, None),
        ),
        check_vma=False,
    )
```

```python
import functools

import jax
import jax.numpy as jnp
from jax import lax
from jax.experimental import pallas as pl
from jax.experimental.pallas import tpu as pltpu
from jax.sharding import Mesh, PartitionSpec as P


BF = jnp.bfloat16
F32 = jnp.float32
DP = ("x", "z")
GROUP = ("y", "c")


def shift(a, step):
    return lax.ppermute(a, "y", [(i, (i + step) % 4) for i in range(4)])


def swap(a):
    return lax.ppermute(a, "c", [(0, 1), (1, 0)])


def spread(left, right):
    half = left.shape[0] // 2
    return jnp.concatenate([shift(left[:half], 1), shift(right[half:], -1)], axis=0)


def tdot(a, b):
    return lax.dot_general(a, b, (((0,), (0,)), ((), ())), preferred_element_type=F32)


def dot_t(a, b):
    return lax.dot_general(a, b, (((1,), (1,)), ((), ())), preferred_element_type=F32)


def send_each(a):
    return lax.all_to_all(a, GROUP, split_axis=0, concat_axis=0, tiled=True)


def ring_all(a, axis):
    others = [lax.ppermute(a, axis, [(i, (i + k) % 4) for i in range(4)]) for k in (1, 2, 3)]
    return a + others[0] + others[1] + others[2]


LANES = 128


def grad_kernel(tiles, gate_a, gate_b, up_a, up_b, w_ref, xa_ref, xb_ref, dy_ref, prob_ref,
                parts_ref, pre_ref, score_ref, hid, dyk, x):
    i = pl.program_id(0)
    ff = hid.shape[1]
    tile = gate_a.shape[1]
    split = xa_ref.shape[0]

    @pl.when(i == 0)
    def _():
        score_ref[...] = jnp.zeros_like(score_ref)
        dyk[...] = (prob_ref[...] * dy_ref[...].astype(F32)).astype(BF)
        x[:split, :] = xa_ref[...]
        x[split:, :] = xb_ref[...]

    @pl.when(i < tiles)
    def _():
        at = pl.multiple_of(i * tile, tile)
        raw = lax.dot_general(dy_ref[...], w_ref[...], (((1,), (1,)), ((), ())), preferred_element_type=F32)
        gate = jnp.concatenate([gate_a[...], gate_b[...]], axis=0)
        up = jnp.concatenate([up_a[...], up_b[...]], axis=0)
        sig = 1.0 / (1.0 + jnp.exp(-gate))
        silu = gate * sig
        hidden = (silu * up).astype(BF)
        score_ref[...] += jnp.sum(hidden.astype(F32) * raw, axis=1, keepdims=True)
        grad = prob_ref[...] * raw
        hid[:, pl.ds(at, tile)] = hidden
        pre_ref[:, pl.ds(at, tile)] = (grad * up * sig * (1.0 + gate * (1.0 - sig))).astype(BF)
        pre_ref[:, pl.ds(pl.multiple_of(ff + at, tile), tile)] = (grad * silu).astype(BF)

    def emit(left, right, base, r):
        cols = 512 if right.shape[1] % 512 == 0 else right.shape[1]
        for q in range(right.shape[1] // cols):
            g = jnp.dot(left, right[:, q * cols : (q + 1) * cols], preferred_element_type=F32).astype(BF)
            for t in range(cols // LANES):
                at = base + (q * (cols // LANES) + t) * r
                for d in range(4):
                    parts_ref[d, at : at + r, :] = g[d * r : (d + 1) * r, t * LANES : (t + 1) * LANES]

    @pl.when(i >= tiles)
    def _():
        k = i - tiles
        r = x.shape[1] // 16
        emit(x[:, pl.ds(pl.multiple_of(k * 4 * r, 4 * r), 4 * r)].T, pre_ref, 0, r)
        base = 2 * ff // LANES * r
        r = ff // 16
        emit(hid[:, pl.ds(pl.multiple_of(k * 4 * r, 4 * r), 4 * r)].T, dyk, base, r)


def weight_grads(act_a, act_b, w_dn, xa, xb, dy, row_prob):
    rows, width = dy.shape
    ff = w_dn.shape[0]
    tiles = 6
    tile = ff // tiles
    depth = (2 * ff * (width // 16) + width * (ff // 16)) // LANES
    na, nb = xa.shape[0], xb.shape[0]
    last = tiles - 1
    whole = lambda i: (0, 0)
    low = lambda i: (0, jnp.minimum(i, last))
    high = lambda i: (0, tiles + jnp.minimum(i, last))
    return pl.pallas_call(
        functools.partial(grad_kernel, tiles),
        grid=(tiles + 4,),
        in_specs=[
            pl.BlockSpec((na, tile), low),
            pl.BlockSpec((nb, tile), low),
            pl.BlockSpec((na, tile), high),
            pl.BlockSpec((nb, tile), high),
            pl.BlockSpec((tile, width), lambda i: (jnp.minimum(i, last), 0)),
            pl.BlockSpec((na, width), whole),
            pl.BlockSpec((nb, width), whole),
            pl.BlockSpec((rows, width), whole),
            pl.BlockSpec((rows, 1), whole),
        ],
        out_specs=[
            pl.BlockSpec((4, depth, LANES), lambda i: (jnp.maximum(i - tiles, 0), 0, 0)),
            pl.BlockSpec((rows, 2 * ff), whole),
            pl.BlockSpec((rows, 1), whole),
        ],
        out_shape=[
            jax.ShapeDtypeStruct((16, depth, LANES), BF),
            pltpu.HBM((rows, 2 * ff), BF),
            jax.ShapeDtypeStruct((rows, 1), F32),
        ],
        scratch_shapes=[
            pltpu.VMEM((rows, ff), BF),
            pltpu.VMEM((rows, width), BF),
            pltpu.VMEM((rows, width), BF),
        ],
        compiler_params=pltpu.CompilerParams(vmem_limit_bytes=36 * 2**20),
        cost_estimate=pl.CostEstimate(
            flops=2 * rows * width * ff * 4, bytes_accessed=36 * 2**20, transcendentals=rows * ff
        ),
        name="weight_grads",
    )(act_a, act_b, act_a, act_b, w_dn, xa, xb, dy, row_prob)


def unpack_kernel(in_ref, gu_ref, dn_ref):
    at = 0
    for ref in (gu_ref, dn_ref):
        r = ref.shape[0]
        for t in range(ref.shape[1] // LANES):
            ref[:, t * LANES : (t + 1) * LANES] = in_ref[at : at + r, :]
            at += r


def unpack(total, width, ff):
    return pl.pallas_call(
        unpack_kernel,
        out_shape=[
            jax.ShapeDtypeStruct((width // 16, 2 * ff), BF),
            jax.ShapeDtypeStruct((ff // 16, width), BF),
        ],
        name="unpack",
    )(total)


def step(tokens, out_grad, z_weight, router_weight, expert_ids, gate_up_weight, down_weight):
    tok, width = tokens.shape
    routed = router_weight.shape[1]
    cap = tok // 2
    w_gu = gate_up_weight[0]
    w_dn = down_weight[0]
    ff = w_dn.shape[0]
    my_y = lax.axis_index("y")
    my_c = lax.axis_index("c")

    names = jnp.arange(routed, dtype=jnp.int32)[None, :]
    slots = jnp.arange(cap, dtype=F32)[None, :, None]
    before = (jnp.arange(tok)[:, None] < jnp.arange(tok)[None, :]).astype(BF)
    top = expert_ids.shape[1]
    id_row = expert_ids.T.astype(BF).reshape(1, top * tok)
    x0 = jnp.concatenate([tokens, jnp.pad(id_row, ((0, 7), (0, width - top * tok)))], axis=0)
    logits = jnp.dot(tokens, router_weight, preferred_element_type=F32)
    chosen = expert_ids[:, 0:1] == names
    for k in range(1, top):
        chosen = chosen | (expert_ids[:, k : k + 1] == names)
    expl = jnp.exp(logits)
    sel_exp = jnp.where(chosen, expl, 0.0)
    probs = jnp.where(chosen, sel_exp / jnp.sum(sel_exp, axis=1, keepdims=True), 0.0)
    log_total = jnp.log(jnp.sum(expl, axis=1, keepdims=True))
    mine = probs[:, :8].T
    high = mine.astype(BF)
    low = (mine - high.astype(F32)).astype(BF)
    prob_row = jnp.concatenate([high.reshape(1, 8 * tok), low.reshape(1, 8 * tok)], axis=1)
    g0 = jnp.concatenate([out_grad, jnp.pad(prob_row, ((0, 7), (0, width - 16 * tok)))], axis=0)

    x1, x3 = shift(x0, 1), shift(x0, -1)
    g1, g3 = shift(g0, 1), shift(g0, -1)
    x2 = spread(x1, x3)
    g2 = spread(g1, g3)
    x_parts, g_parts = [], []
    for part in (x0, x1, x3, x2):
        x_parts += [part, swap(part)]
    for part in (g0, g1, g3, g2):
        g_parts += [part, swap(part)]
    gray = lambda k: k ^ (k >> 1)
    place = [gray((my_y - s // 2) % 4) * 2 + (my_c ^ (s % 2)) for s in range(8)]
    origin = [((my_y - gray(k)) % 4) * 2 + (my_c ^ cc) for k in range(4) for cc in range(2)]

    me = my_y * 2 + my_c

    def choose(parts):
        named = jnp.stack([p[tok, : top * tok].reshape(top, tok) for p in parts])
        member = jnp.max(jnp.where(named == me.astype(BF), 1.0, 0.0), axis=1)
        rank = jnp.dot(member.astype(BF), before, preferred_element_type=F32)
        return (rank[:, None, :] == slots) & (member[:, None, :] > 0.0)

    def compact(take, parts):
        rows = [
            jnp.dot(take[j].astype(BF), p[:tok], preferred_element_type=F32).astype(BF)
            for j, p in enumerate(parts)
        ]
        return jnp.concatenate(rows, axis=0)

    take_a = choose(x_parts[:6])
    xa = compact(take_a, x_parts[:6])
    act_a = jnp.dot(xa, w_gu, preferred_element_type=F32)
    take_b = choose(x_parts[6:])
    xb = compact(take_b, x_parts[6:])
    act_b = jnp.dot(xb, w_gu, preferred_element_type=F32)
    take = jnp.concatenate([take_a, take_b], axis=0)
    pick = (jnp.arange(16, dtype=jnp.int32) % 8 == me)[None, :, None]
    pairs = jnp.stack([p[tok, : 16 * tok].reshape(16, tok) for p in g_parts]).astype(F32)
    prob_of = jnp.sum(jnp.where(pick, pairs, 0.0), axis=1)
    row_prob = jnp.sum(jnp.where(take, prob_of[:, None, :], 0.0), axis=2).reshape(8 * cap, 1)
    dy = compact(take, g_parts)
    parts, pre, score = weight_grads(act_a, act_b, w_dn, xa, xb, dy, row_prob)
    total = lax.psum_scatter(parts.reshape(1, -1, parts.shape[2]), DP, scatter_dimension=1, tiled=True)[0]
    gate_up_grad, down_grad = unpack(total, width, ff)

    home_score = send_each(jnp.concatenate(
        [lax.dynamic_slice_in_dim(score.reshape(8, 1, cap), s, 1, 0) for s in place], axis=0))
    row_grad = dot_t(pre, w_gu).astype(BF)
    row_grad = row_grad.reshape(8, cap, width)
    home_rows = send_each(jnp.concatenate(
        [lax.dynamic_slice_in_dim(row_grad, s, 1, 0) for s in place], axis=0))

    member = jnp.where(chosen[:, :8], 1.0, 0.0).T
    rank = jnp.dot(member.astype(BF), before, preferred_element_type=F32)
    back = (rank[:, None, :] == slots) & (member[:, None, :] > 0.0)
    score_of = jnp.sum(jnp.where(back, home_score.reshape(8, cap, 1), 0.0), axis=1)
    scores = jnp.concatenate([score_of.T, jnp.zeros((tok, routed - 8), F32)], axis=1)
    mean_score = jnp.sum(probs * scores, axis=1, keepdims=True)
    z_grad = 2.0 * z_weight[:, None] * log_total * jnp.exp(logits - log_total)
    logit_grad = (z_grad + probs * (scores - mean_score)).astype(BF)
    share = send_each(logit_grad.T.reshape(8, routed // 8, tok))
    share = jnp.concatenate([lax.dynamic_slice_in_dim(share, o, 1, 0)[0] for o in origin], axis=1)
    group_tokens = jnp.concatenate([p[:tok] for p in x_parts], axis=0)
    router_part = jnp.dot(share, group_tokens, preferred_element_type=F32)
    router_part = ring_all(ring_all(router_part, "x"), "z")
    near = lax.all_gather(router_part, "y", axis=0, tiled=False)
    away = swap(near)
    both = jnp.stack([jnp.where(my_c == 0, near, away), jnp.where(my_c == 0, away, near)], axis=1)
    router_grad = both.reshape(routed, width).T
    token_grad = (
        tdot(back.astype(BF).reshape(8 * cap, tok), home_rows.reshape(8 * cap, width))
        + dot_t(logit_grad, router_weight)
    ).astype(BF)
    return token_grad, router_grad, gate_up_grad[None], down_grad[None]


def solution(mesh):
    grid = Mesh(mesh.devices.reshape(4, 4, 4, 2), ("x", "z", "y", "c"))
    every = ("x", "z", "y", "c")
    return jax.shard_map(
        step,
        mesh=grid,
        in_specs=(
            P(every, None),
            P(every, None),
            P(every),
            P(),
            P(every, None),
            P(GROUP, None, None),
            P(GROUP, None, None),
        ),
        out_specs=(
            P(every, None),
            P(),
            P(GROUP, DP, None),
            P(GROUP, DP, None),
        ),
        check_vma=False,
    )
```

```python
import jax
import jax.numpy as jnp
from jax import lax
from jax.experimental import pallas as pl
from jax.experimental.pallas import tpu as pltpu
from jax.sharding import Mesh, PartitionSpec as P


BF = jnp.bfloat16
F32 = jnp.float32
DP = ("x", "z")
GROUP = ("y", "c")


def shift(a, step):
    return lax.ppermute(a, "y", [(i, (i + step) % 4) for i in range(4)])


def swap(a):
    return lax.ppermute(a, "c", [(0, 1), (1, 0)])


def spread(left, right):
    half = left.shape[0] // 2
    left, right = left[:half], right[half:]
    return jnp.concatenate([shift(left, 1), shift(right, -1)], axis=0)


def tdot(a, b):
    return lax.dot_general(a, b, (((0,), (0,)), ((), ())), preferred_element_type=F32)


def dot_t(a, b):
    return lax.dot_general(a, b, (((1,), (1,)), ((), ())), preferred_element_type=F32)


def send_each(a):
    return lax.all_to_all(a, GROUP, split_axis=0, concat_axis=0, tiled=True)


def ring_all(a, axis):
    others = [lax.ppermute(a, axis, [(i, (i + k) % 4) for i in range(4)]) for k in (1, 2, 3)]
    return a + others[0] + others[1] + others[2]


LANES = 128


def in_hbm(a):
    return pltpu.with_memory_space_constraint(a, pltpu.HBM)


TILES = 6


def gate_kernel(x_ref, gate_ref, up_ref, hid_ref, slope_ref, silu_ref):
    x = x_ref[...]
    gate = jnp.dot(x, gate_ref[...], preferred_element_type=F32)
    up = jnp.dot(x, up_ref[...], preferred_element_type=F32)
    sig = 1.0 / (1.0 + jnp.exp(-gate))
    silu = gate * sig
    hid_ref[...] = (silu * up).astype(BF)
    slope_ref[...] = (up * sig * (1.0 + gate * (1.0 - sig))).astype(BF)
    silu_ref[...] = silu.astype(BF)


def gate_up(x, w):
    rows, width = x.shape
    ff = w.shape[1] // 2
    tile = ff // TILES
    w = in_hbm(w)
    return pl.pallas_call(
        gate_kernel,
        grid=(TILES,),
        in_specs=[
            pl.BlockSpec((rows, width), lambda i: (0, 0)),
            pl.BlockSpec((width, tile), lambda i: (0, i)),
            pl.BlockSpec((width, tile), lambda i: (0, TILES + i)),
        ],
        out_specs=[pl.BlockSpec((rows, tile), lambda i: (0, i))] * 3,
        out_shape=[pltpu.HBM((rows, ff), BF)] * 3,
        compiler_params=pltpu.CompilerParams(vmem_limit_bytes=20 * 2**20),
        cost_estimate=pl.CostEstimate(
            flops=4 * rows * width * ff, bytes_accessed=2 * w.size, transcendentals=rows * ff
        ),
        name="gate_up",
    )(x, w, w)


def grad_kernel(hid_ref, slope_ref, silu_ref, w_ref, x, dy_ref, prob_ref,
                parts_ref, pre_ref, score_ref, dyk, hid):
    i = pl.program_id(0)
    ff = hid.shape[1]
    tile = ff // TILES

    @pl.when(i == 0)
    def _():
        score_ref[...] = jnp.zeros_like(score_ref)
        dyk[...] = (prob_ref[...] * dy_ref[...].astype(F32)).astype(BF)

    @pl.when(i < TILES)
    def _():
        at = pl.multiple_of(i * tile, tile)
        raw = lax.dot_general(dy_ref[...], w_ref[...], (((1,), (1,)), ((), ())), preferred_element_type=F32)
        hidden = hid_ref[...]
        score_ref[...] += jnp.sum(hidden.astype(F32) * raw, axis=1, keepdims=True)
        grad = prob_ref[...] * raw
        hid[:, pl.ds(at, tile)] = hidden
        pre_ref[:, pl.ds(at, tile)] = (grad * slope_ref[...].astype(F32)).astype(BF)
        pre_ref[:, pl.ds(pl.multiple_of(ff + at, tile), tile)] = (grad * silu_ref[...].astype(F32)).astype(BF)

    def emit(left, right, base, r):
        cols = 512 if right.shape[1] % 512 == 0 else right.shape[1]
        for q in range(right.shape[1] // cols):
            g = jnp.dot(left, right[:, q * cols : (q + 1) * cols], preferred_element_type=F32).astype(BF)
            for t in range(cols // LANES):
                at = base + (q * (cols // LANES) + t) * r
                for d in range(4):
                    parts_ref[d, at : at + r, :] = g[d * r : (d + 1) * r, t * LANES : (t + 1) * LANES]

    @pl.when(i >= TILES)
    def _():
        k = i - TILES
        r = x.shape[1] // 16
        emit(x[:, pl.ds(pl.multiple_of(k * 4 * r, 4 * r), 4 * r)].T, pre_ref, 0, r)
        base = 2 * ff // LANES * r
        r = ff // 16
        emit(hid[:, pl.ds(pl.multiple_of(k * 4 * r, 4 * r), 4 * r)].T, dyk, base, r)


def weight_grads(acts, w_dn, x, dy, row_prob):
    rows, width = dy.shape
    ff = w_dn.shape[0]
    tile = ff // TILES
    depth = (2 * ff * (width // 16) + width * (ff // 16)) // LANES
    last = TILES - 1
    whole = lambda i: (0, 0)
    across = pl.BlockSpec((rows, tile), lambda i: (0, jnp.minimum(i, last)))
    return pl.pallas_call(
        grad_kernel,
        grid=(TILES + 4,),
        in_specs=[
            across,
            across,
            across,
            pl.BlockSpec((tile, width), lambda i: (jnp.minimum(i, last), 0)),
            pl.BlockSpec((rows, width), whole),
            pl.BlockSpec((rows, width), whole),
            pl.BlockSpec((rows, 1), whole),
        ],
        out_specs=[
            pl.BlockSpec((4, depth, LANES), lambda i: (jnp.maximum(i - TILES, 0), 0, 0)),
            pl.BlockSpec((rows, 2 * ff), whole),
            pl.BlockSpec((rows, 1), whole),
        ],
        out_shape=[
            jax.ShapeDtypeStruct((16, depth, LANES), BF),
            pltpu.HBM((rows, 2 * ff), BF),
            jax.ShapeDtypeStruct((rows, 1), F32),
        ],
        scratch_shapes=[
            pltpu.VMEM((rows, width), BF),
            pltpu.VMEM((rows, ff), BF),
        ],
        compiler_params=pltpu.CompilerParams(vmem_limit_bytes=36 * 2**20),
        cost_estimate=pl.CostEstimate(
            flops=2 * rows * width * ff * 4, bytes_accessed=36 * 2**20, transcendentals=0
        ),
        name="weight_grads",
    )(*[in_hbm(v) for v in acts], in_hbm(w_dn), in_hbm(x), dy, row_prob)


def unpack_kernel(in_ref, gu_ref, dn_ref):
    at = 0
    for ref in (gu_ref, dn_ref):
        r = ref.shape[0]
        for t in range(ref.shape[1] // LANES):
            ref[:, t * LANES : (t + 1) * LANES] = in_ref[at : at + r, :]
            at += r


def unpack(total, width, ff):
    return pl.pallas_call(
        unpack_kernel,
        out_shape=[
            jax.ShapeDtypeStruct((width // 16, 2 * ff), BF),
            jax.ShapeDtypeStruct((ff // 16, width), BF),
        ],
        compiler_params=pltpu.CompilerParams(vmem_limit_bytes=8 * 2**20),
        name="unpack",
    )(total)


def step(tokens, out_grad, z_weight, router_weight, expert_ids, gate_up_weight, down_weight):
    tok, width = tokens.shape
    routed = router_weight.shape[1]
    cap = tok // 2
    w_gu = gate_up_weight[0]
    w_dn = down_weight[0]
    ff = w_dn.shape[0]
    my_y = lax.axis_index("y")
    my_c = lax.axis_index("c")

    names = jnp.arange(routed, dtype=jnp.int32)[None, :]
    slots = jnp.arange(cap, dtype=F32)[None, :, None]
    before = (jnp.arange(tok)[:, None] < jnp.arange(tok)[None, :]).astype(BF)
    top = expert_ids.shape[1]
    id_row = expert_ids.T.astype(BF).reshape(1, top * tok)
    x0 = jnp.concatenate([tokens, jnp.pad(id_row, ((0, 7), (0, width - top * tok)))], axis=0)
    logits = jnp.dot(tokens, router_weight, preferred_element_type=F32)
    chosen = expert_ids[:, 0:1] == names
    for k in range(1, top):
        chosen = chosen | (expert_ids[:, k : k + 1] == names)
    expl = jnp.exp(logits)
    sel_exp = jnp.where(chosen, expl, 0.0)
    probs = jnp.where(chosen, sel_exp / jnp.sum(sel_exp, axis=1, keepdims=True), 0.0)
    log_total = jnp.log(jnp.sum(expl, axis=1, keepdims=True))
    mine = probs[:, :8].T
    high = mine.astype(BF)
    low = (mine - high.astype(F32)).astype(BF)
    prob_row = jnp.concatenate([high.reshape(1, 8 * tok), low.reshape(1, 8 * tok)], axis=1)
    g0 = jnp.concatenate([out_grad, jnp.pad(prob_row, ((0, 7), (0, width - 16 * tok)))], axis=0)

    x1, x3 = shift(x0, 1), shift(x0, -1)
    g1, g3 = shift(g0, 1), shift(g0, -1)
    x2 = spread(x1, x3)
    g2 = spread(g1, g3)
    x_parts, g_parts = [], []
    for part in (x0, x1, x3, x2):
        x_parts += [part, swap(part)]
    for part in (g0, g1, g3, g2):
        g_parts += [part, swap(part)]
    gray = lambda k: k ^ (k >> 1)
    place = [gray((my_y - s // 2) % 4) * 2 + (my_c ^ (s % 2)) for s in range(8)]
    origin = [((my_y - gray(k)) % 4) * 2 + (my_c ^ cc) for k in range(4) for cc in range(2)]

    me = my_y * 2 + my_c

    def choose(parts):
        named = jnp.stack([p[tok, : top * tok].reshape(top, tok) for p in parts])
        member = jnp.max(jnp.where(named == me.astype(BF), 1.0, 0.0), axis=1)
        rank = jnp.dot(member.astype(BF), before, preferred_element_type=F32)
        return (rank[:, None, :] == slots) & (member[:, None, :] > 0.0)

    def compact(take, parts):
        rows = [
            jnp.dot(take[j].astype(BF), p[:tok], preferred_element_type=F32).astype(BF)
            for j, p in enumerate(parts)
        ]
        return jnp.concatenate(rows, axis=0)

    take_a = choose(x_parts[:6])
    xa = compact(take_a, x_parts[:6])
    take_b = choose(x_parts[6:])
    xb = compact(take_b, x_parts[6:])
    x = jnp.concatenate([xa, xb], axis=0)
    acts = gate_up(x, w_gu)
    take = jnp.concatenate([take_a, take_b], axis=0)
    pick = (jnp.arange(16, dtype=jnp.int32) % 8 == me)[None, :, None]
    pairs = jnp.stack([p[tok, : 16 * tok].reshape(16, tok) for p in g_parts]).astype(F32)
    prob_of = jnp.sum(jnp.where(pick, pairs, 0.0), axis=1)
    row_prob = jnp.sum(jnp.where(take, prob_of[:, None, :], 0.0), axis=2).reshape(8 * cap, 1)
    dy = compact(take, g_parts)
    parts, pre, score = weight_grads(acts, w_dn, x, dy, row_prob)
    total = lax.psum_scatter(parts.reshape(1, -1, parts.shape[2]), DP, scatter_dimension=1, tiled=True)[0]
    gate_up_grad, down_grad = unpack(total, width, ff)

    home_score = send_each(jnp.concatenate(
        [lax.dynamic_slice_in_dim(score.reshape(8, 1, cap), s, 1, 0) for s in place], axis=0))
    row_grad = dot_t(pre, w_gu).astype(BF)
    row_grad = row_grad.reshape(8, cap, width)
    home_rows = send_each(jnp.concatenate(
        [lax.dynamic_slice_in_dim(row_grad, s, 1, 0) for s in place], axis=0))

    member = jnp.where(chosen[:, :8], 1.0, 0.0).T
    rank = jnp.dot(member.astype(BF), before, preferred_element_type=F32)
    back = (rank[:, None, :] == slots) & (member[:, None, :] > 0.0)
    score_of = jnp.sum(jnp.where(back, home_score.reshape(8, cap, 1), 0.0), axis=1)
    scores = jnp.concatenate([score_of.T, jnp.zeros((tok, routed - 8), F32)], axis=1)
    mean_score = jnp.sum(probs * scores, axis=1, keepdims=True)
    z_grad = 2.0 * z_weight[:, None] * log_total * jnp.exp(logits - log_total)
    logit_grad = (z_grad + probs * (scores - mean_score)).astype(BF)
    share = send_each(logit_grad.T.reshape(8, routed // 8, tok))
    share = jnp.concatenate([lax.dynamic_slice_in_dim(share, o, 1, 0)[0] for o in origin], axis=1)
    group_tokens = jnp.concatenate([p[:tok] for p in x_parts], axis=0)
    router_part = jnp.dot(share, group_tokens, preferred_element_type=F32)
    router_part = ring_all(ring_all(router_part, "x"), "z")
    near = lax.all_gather(router_part, "y", axis=0, tiled=False)
    away = swap(near)
    both = jnp.stack([jnp.where(my_c == 0, near, away), jnp.where(my_c == 0, away, near)], axis=1)
    router_grad = both.reshape(routed, width).T
    token_grad = (
        tdot(back.astype(BF).reshape(8 * cap, tok), home_rows.reshape(8 * cap, width))
        + dot_t(logit_grad, router_weight)
    ).astype(BF)
    return token_grad, router_grad, gate_up_grad[None], down_grad[None]


def solution(mesh):
    grid = Mesh(mesh.devices.reshape(4, 4, 4, 2), ("x", "z", "y", "c"))
    every = ("x", "z", "y", "c")
    return jax.shard_map(
        step,
        mesh=grid,
        in_specs=(
            P(every, None),
            P(every, None),
            P(every),
            P(),
            P(every, None),
            P(GROUP, None, None),
            P(GROUP, None, None),
        ),
        out_specs=(
            P(every, None),
            P(),
            P(GROUP, DP, None),
            P(GROUP, DP, None),
        ),
        check_vma=False,
    )
```

```python
import jax
import jax.numpy as jnp
from jax import lax
from jax.experimental import pallas as pl
from jax.experimental.pallas import tpu as pltpu
from jax.sharding import Mesh, PartitionSpec as P


BF = jnp.bfloat16
F32 = jnp.float32
DP = ("x", "z")
GROUP = ("y", "c")


def shift(a, step):
    return lax.ppermute(a, "y", [(i, (i + step) % 4) for i in range(4)])


def swap(a):
    return lax.ppermute(a, "c", [(0, 1), (1, 0)])


def spread(left, right):
    half = left.shape[0] // 16 * 8
    left, right = left[:half], right[half:]
    return jnp.concatenate([shift(left, 1), shift(right, -1)], axis=0)


def tdot(a, b):
    return lax.dot_general(a, b, (((0,), (0,)), ((), ())), preferred_element_type=F32)


def dot_t(a, b):
    return lax.dot_general(a, b, (((1,), (1,)), ((), ())), preferred_element_type=F32)


def send_each(a):
    return lax.all_to_all(a, GROUP, split_axis=0, concat_axis=0, tiled=True)


def ring_all(a, axis):
    others = [lax.ppermute(a, axis, [(i, (i + k) % 4) for i in range(4)]) for k in (1, 2, 3)]
    return a + others[0] + others[1] + others[2]


LANES = 128


def in_hbm(a):
    return pltpu.with_memory_space_constraint(a, pltpu.HBM)


TILES = 6


def expert_kernel(w_gate, w_up, w_dn, x, dy, prob_ref, parts_ref, pre_hbm, score_ref, dyk, hid, pre, sem):
    i = pl.program_id(0)
    ff = hid.shape[1]
    tile = ff // TILES
    store = pltpu.make_async_copy(pre, pre_hbm, sem)

    @pl.when(i == 0)
    def _():
        score_ref[...] = jnp.zeros_like(score_ref)
        dyk[...] = (prob_ref[...] * dy[...].astype(F32)).astype(BF)

    @pl.when(i < TILES)
    def _():
        here = pl.ds(pl.multiple_of(i * tile, tile), tile)
        there = pl.ds(pl.multiple_of(ff + i * tile, tile), tile)
        rows = x[...]
        gate = jnp.dot(rows, w_gate[...], preferred_element_type=F32)
        up = jnp.dot(rows, w_up[...], preferred_element_type=F32)
        raw = lax.dot_general(dy[...], w_dn[...], (((1,), (1,)), ((), ())), preferred_element_type=F32)
        sig = 1.0 / (1.0 + jnp.exp(-gate))
        silu = gate * sig
        hidden = (silu * up).astype(BF)
        score_ref[...] += jnp.sum(hidden.astype(F32) * raw, axis=1, keepdims=True)
        grad = prob_ref[...] * raw
        hid[:, here] = hidden
        pre[:, here] = (grad * up * sig * (1.0 + gate * (1.0 - sig))).astype(BF)
        pre[:, there] = (grad * silu).astype(BF)

    def emit(left, right, base, r):
        cols = 512 if right.shape[1] % 512 == 0 else right.shape[1]
        for q in range(right.shape[1] // cols):
            g = jnp.dot(left, right[:, q * cols : (q + 1) * cols], preferred_element_type=F32).astype(BF)
            for t in range(cols // LANES):
                at = base + (q * (cols // LANES) + t) * r
                for d in range(4):
                    parts_ref[d, at : at + r, :] = g[d * r : (d + 1) * r, t * LANES : (t + 1) * LANES]

    @pl.when(i == TILES)
    def _():
        store.start()

    @pl.when(i >= TILES)
    def _():
        k = i - TILES
        r = x.shape[1] // 16
        emit(x[:, pl.ds(pl.multiple_of(k * 4 * r, 4 * r), 4 * r)].T, pre, 0, r)
        base = 2 * ff // LANES * r
        r = ff // 16
        emit(hid[:, pl.ds(pl.multiple_of(k * 4 * r, 4 * r), 4 * r)].T, dyk, base, r)

    @pl.when(i == TILES + 3)
    def _():
        store.wait()


def expert_grads(w_gu, w_dn, x, dy, row_prob):
    rows, width = dy.shape
    ff = w_dn.shape[0]
    depth = (2 * ff * (width // 16) + width * (ff // 16)) // LANES
    tile, last = ff // TILES, TILES - 1
    whole = lambda i: (0, 0)
    w_gu = in_hbm(w_gu)
    return pl.pallas_call(
        expert_kernel,
        grid=(TILES + 4,),
        in_specs=[
            pl.BlockSpec((width, tile), lambda i: (0, jnp.minimum(i, last))),
            pl.BlockSpec((width, tile), lambda i: (0, TILES + jnp.minimum(i, last))),
            pl.BlockSpec((tile, width), lambda i: (jnp.minimum(i, last), 0)),
        ]
        + [pl.BlockSpec((rows, width), whole, pipeline_mode=pl.Buffered(1))] * 2
        + [pl.BlockSpec((rows, 1), whole)],
        out_specs=[
            pl.BlockSpec((4, depth, LANES), lambda i: (jnp.maximum(i - TILES, 0), 0, 0)),
            pl.BlockSpec(memory_space=pltpu.HBM),
            pl.BlockSpec((rows, 1), whole),
        ],
        out_shape=[
            jax.ShapeDtypeStruct((16, depth, LANES), BF),
            pltpu.HBM((rows, 2 * ff), BF),
            jax.ShapeDtypeStruct((rows, 1), F32),
        ],
        scratch_shapes=[
            pltpu.VMEM((rows, width), BF),
            pltpu.VMEM((rows, ff), BF),
            pltpu.VMEM((rows, 2 * ff), BF),
            pltpu.SemaphoreType.DMA,
        ],
        compiler_params=pltpu.CompilerParams(vmem_limit_bytes=36 * 2**20),
        cost_estimate=pl.CostEstimate(
            flops=16 * rows * width * ff, bytes_accessed=40 * 2**20, transcendentals=rows * ff
        ),
        name="expert_grads",
    )(w_gu, w_gu, in_hbm(w_dn), in_hbm(x), in_hbm(dy), row_prob)


def unpack_kernel(in_ref, gu_ref, dn_ref):
    at = 0
    for ref in (gu_ref, dn_ref):
        r = ref.shape[0]
        for t in range(ref.shape[1] // LANES):
            ref[:, t * LANES : (t + 1) * LANES] = in_ref[at : at + r, :]
            at += r


def unpack(total, width, ff):
    return pl.pallas_call(
        unpack_kernel,
        out_shape=[
            jax.ShapeDtypeStruct((width // 16, 2 * ff), BF),
            jax.ShapeDtypeStruct((ff // 16, width), BF),
        ],
        compiler_params=pltpu.CompilerParams(vmem_limit_bytes=8 * 2**20),
        name="unpack",
    )(total)


def step(tokens, out_grad, z_weight, router_weight, expert_ids, gate_up_weight, down_weight):
    tok, width = tokens.shape
    routed = router_weight.shape[1]
    cap = tok // 2
    w_gu = gate_up_weight[0]
    w_dn = down_weight[0]
    ff = w_dn.shape[0]
    my_y = lax.axis_index("y")
    my_c = lax.axis_index("c")

    names = jnp.arange(routed, dtype=jnp.int32)[None, :]
    slots = jnp.arange(cap, dtype=F32)[None, :, None]
    before = (jnp.arange(tok)[:, None] < jnp.arange(tok)[None, :]).astype(BF)
    top = expert_ids.shape[1]
    id_row = expert_ids.T.astype(BF).reshape(1, top * tok)
    x0 = jnp.concatenate([tokens, jnp.pad(id_row, ((0, 7), (0, width - top * tok)))], axis=0)
    logits = jnp.dot(tokens, router_weight, preferred_element_type=F32)
    chosen = expert_ids[:, 0:1] == names
    for k in range(1, top):
        chosen = chosen | (expert_ids[:, k : k + 1] == names)
    expl = jnp.exp(logits)
    sel_exp = jnp.where(chosen, expl, 0.0)
    probs = jnp.where(chosen, sel_exp / jnp.sum(sel_exp, axis=1, keepdims=True), 0.0)
    log_total = jnp.log(jnp.sum(expl, axis=1, keepdims=True))
    mine = probs[:, :8].T
    high = mine.astype(BF)
    low = (mine - high.astype(F32)).astype(BF)
    prob_row = jnp.concatenate([high.reshape(1, 8 * tok), low.reshape(1, 8 * tok)], axis=1)
    g0 = jnp.concatenate([out_grad, jnp.pad(prob_row, ((0, 7), (0, width - 16 * tok)))], axis=0)

    x1, x3 = shift(x0, 1), shift(x0, -1)
    g1, g3 = shift(g0, 1), shift(g0, -1)
    x2 = spread(x1, x3)
    g2 = spread(g1, g3)
    x_parts, g_parts = [], []
    for part in (x0, x1, x3, x2):
        x_parts += [part, swap(part)]
    for part in (g0, g1, g3, g2):
        g_parts += [part, swap(part)]
    gray = lambda k: k ^ (k >> 1)
    place = [gray((my_y - s // 2) % 4) * 2 + (my_c ^ (s % 2)) for s in range(8)]
    origin = [((my_y - gray(k)) % 4) * 2 + (my_c ^ cc) for k in range(4) for cc in range(2)]

    me = my_y * 2 + my_c

    def choose(parts):
        named = jnp.stack([p[tok, : top * tok].reshape(top, tok) for p in parts])
        member = jnp.max(jnp.where(named == me.astype(BF), 1.0, 0.0), axis=1)
        rank = jnp.dot(member.astype(BF), before, preferred_element_type=F32)
        return (rank[:, None, :] == slots) & (member[:, None, :] > 0.0)

    def compact(take, parts):
        rows = [
            jnp.dot(take[j].astype(BF), p[:tok], preferred_element_type=F32).astype(BF)
            for j, p in enumerate(parts)
        ]
        return jnp.concatenate(rows, axis=0)

    take_a = choose(x_parts[:6])
    xa = compact(take_a, x_parts[:6])
    take_b = choose(x_parts[6:])
    xb = compact(take_b, x_parts[6:])
    x = jnp.concatenate([xa, xb], axis=0)
    take = jnp.concatenate([take_a, take_b], axis=0)
    pick = (jnp.arange(16, dtype=jnp.int32) % 8 == me)[None, :, None]
    pairs = jnp.stack([p[tok, : 16 * tok].reshape(16, tok) for p in g_parts]).astype(F32)
    prob_of = jnp.sum(jnp.where(pick, pairs, 0.0), axis=1)
    row_prob = jnp.sum(jnp.where(take, prob_of[:, None, :], 0.0), axis=2).reshape(8 * cap, 1)
    dy = compact(take, g_parts)
    parts, pre, score = expert_grads(w_gu, w_dn, x, dy, row_prob)
    total = lax.psum_scatter(parts.reshape(1, -1, parts.shape[2]), DP, scatter_dimension=1, tiled=True)[0]
    gate_up_grad, down_grad = unpack(total, width, ff)

    home_score = send_each(jnp.concatenate(
        [lax.dynamic_slice_in_dim(score.reshape(8, 1, cap), s, 1, 0) for s in place], axis=0))
    row_grad = dot_t(pre, w_gu).astype(BF)
    row_grad = row_grad.reshape(8, cap, width)
    home_rows = send_each(jnp.concatenate(
        [lax.dynamic_slice_in_dim(row_grad, s, 1, 0) for s in place], axis=0))

    member = jnp.where(chosen[:, :8], 1.0, 0.0).T
    rank = jnp.dot(member.astype(BF), before, preferred_element_type=F32)
    back = (rank[:, None, :] == slots) & (member[:, None, :] > 0.0)
    score_of = jnp.sum(jnp.where(back, home_score.reshape(8, cap, 1), 0.0), axis=1)
    scores = jnp.concatenate([score_of.T, jnp.zeros((tok, routed - 8), F32)], axis=1)
    mean_score = jnp.sum(probs * scores, axis=1, keepdims=True)
    z_grad = 2.0 * z_weight[:, None] * log_total * jnp.exp(logits - log_total)
    logit_grad = (z_grad + probs * (scores - mean_score)).astype(BF)
    share = send_each(logit_grad.T.reshape(8, routed // 8, tok))
    share = jnp.concatenate([lax.dynamic_slice_in_dim(share, o, 1, 0)[0] for o in origin], axis=1)
    group_tokens = jnp.concatenate([p[:tok] for p in x_parts], axis=0)
    router_part = jnp.dot(share, group_tokens, preferred_element_type=F32)
    router_part = ring_all(ring_all(router_part, "x"), "z")
    near = lax.all_gather(router_part, "y", axis=0, tiled=False)
    away = swap(near)
    both = jnp.stack([jnp.where(my_c == 0, near, away), jnp.where(my_c == 0, away, near)], axis=1)
    router_grad = both.reshape(routed, width).T
    token_grad = (
        tdot(back.astype(BF).reshape(8 * cap, tok), home_rows.reshape(8 * cap, width))
        + dot_t(logit_grad, router_weight)
    ).astype(BF)
    return token_grad, router_grad, gate_up_grad[None], down_grad[None]


def solution(mesh):
    grid = Mesh(mesh.devices.reshape(4, 4, 4, 2), ("x", "z", "y", "c"))
    every = ("x", "z", "y", "c")
    return jax.shard_map(
        step,
        mesh=grid,
        in_specs=(
            P(every, None),
            P(every, None),
            P(every),
            P(),
            P(every, None),
            P(GROUP, None, None),
            P(GROUP, None, None),
        ),
        out_specs=(
            P(every, None),
            P(),
            P(GROUP, DP, None),
            P(GROUP, DP, None),
        ),
        check_vma=False,
    )
```

```python
import jax
import jax.numpy as jnp
from jax import lax
from jax.experimental import pallas as pl
from jax.experimental.pallas import tpu as pltpu
from jax.sharding import Mesh, PartitionSpec as P


BF = jnp.bfloat16
F32 = jnp.float32
DP = ("x", "z")
GROUP = ("y", "c")


def shift(a, step):
    return lax.ppermute(a, "y", [(i, (i + step) % 4) for i in range(4)])


def swap(a):
    return lax.ppermute(a, "c", [(0, 1), (1, 0)])


def spread(left, right):
    half = left.shape[0] // 16 * 8
    left, right = left[:half], right[half:]
    return jnp.concatenate([shift(left, 1), shift(right, -1)], axis=0)


def tdot(a, b):
    return lax.dot_general(a, b, (((0,), (0,)), ((), ())), preferred_element_type=F32)


def dot_t(a, b):
    return lax.dot_general(a, b, (((1,), (1,)), ((), ())), preferred_element_type=F32)


def send_each(a):
    return lax.all_to_all(a, GROUP, split_axis=0, concat_axis=0, tiled=True)


def ring_all(a, axis):
    sent = a.astype(BF)
    near, far, last = (
        lax.ppermute(sent, axis, [(i, (i + k) % 4) for i in range(4)]).astype(F32) for k in (1, 2, 3)
    )
    return (sent.astype(F32) + far) + (near + last)


LANES = 128


def in_hbm(a):
    return pltpu.with_memory_space_constraint(a, pltpu.HBM)


TILES = 6


def expert_kernel(w_gate, w_up, w_dn, x, dy, prob_ref, parts_ref, pre_hbm, score_ref, dyk, hid, pre, sem):
    i = pl.program_id(0)
    ff = hid.shape[1]
    tile = ff // TILES
    store = pltpu.make_async_copy(pre, pre_hbm, sem)

    @pl.when(i == 0)
    def _():
        score_ref[...] = jnp.zeros_like(score_ref)
        dyk[...] = (prob_ref[...] * dy[...].astype(F32)).astype(BF)

    @pl.when(i < TILES)
    def _():
        here = pl.ds(pl.multiple_of(i * tile, tile), tile)
        there = pl.ds(pl.multiple_of(ff + i * tile, tile), tile)
        rows = x[...]
        gate = jnp.dot(rows, w_gate[...], preferred_element_type=F32)
        up = jnp.dot(rows, w_up[...], preferred_element_type=F32)
        raw = lax.dot_general(dy[...], w_dn[...], (((1,), (1,)), ((), ())), preferred_element_type=F32)
        sig = 1.0 / (1.0 + jnp.exp(-gate))
        silu = gate * sig
        hidden = (silu * up).astype(BF)
        score_ref[...] += jnp.sum(hidden.astype(F32) * raw, axis=1, keepdims=True)
        grad = prob_ref[...] * raw
        hid[:, here] = hidden
        pre[:, here] = (grad * up * sig * (1.0 + gate * (1.0 - sig))).astype(BF)
        pre[:, there] = (grad * silu).astype(BF)

    def emit(left, right, base, r):
        cols = 512 if right.shape[1] % 512 == 0 else right.shape[1]
        for q in range(right.shape[1] // cols):
            g = jnp.dot(left, right[:, q * cols : (q + 1) * cols], preferred_element_type=F32).astype(BF)
            for t in range(cols // LANES):
                at = base + (q * (cols // LANES) + t) * r
                for d in range(4):
                    parts_ref[d, at : at + r, :] = g[d * r : (d + 1) * r, t * LANES : (t + 1) * LANES]

    @pl.when(i == TILES)
    def _():
        store.start()

    @pl.when(i >= TILES)
    def _():
        k = i - TILES
        r = x.shape[1] // 16
        emit(x[:, pl.ds(pl.multiple_of(k * 4 * r, 4 * r), 4 * r)].T, pre, 0, r)
        base = 2 * ff // LANES * r
        r = ff // 16
        emit(hid[:, pl.ds(pl.multiple_of(k * 4 * r, 4 * r), 4 * r)].T, dyk, base, r)

    @pl.when(i == TILES + 3)
    def _():
        store.wait()


def expert_grads(w_gu, w_dn, x, dy, row_prob):
    rows, width = dy.shape
    ff = w_dn.shape[0]
    depth = (2 * ff * (width // 16) + width * (ff // 16)) // LANES
    tile, last = ff // TILES, TILES - 1
    whole = lambda i: (0, 0)
    w_gu = in_hbm(w_gu)
    return pl.pallas_call(
        expert_kernel,
        grid=(TILES + 4,),
        in_specs=[
            pl.BlockSpec((width, tile), lambda i: (0, jnp.minimum(i, last))),
            pl.BlockSpec((width, tile), lambda i: (0, TILES + jnp.minimum(i, last))),
            pl.BlockSpec((tile, width), lambda i: (jnp.minimum(i, last), 0)),
        ]
        + [pl.BlockSpec((rows, width), whole, pipeline_mode=pl.Buffered(1))] * 2
        + [pl.BlockSpec((rows, 1), whole)],
        out_specs=[
            pl.BlockSpec((4, depth, LANES), lambda i: (jnp.maximum(i - TILES, 0), 0, 0)),
            pl.BlockSpec(memory_space=pltpu.HBM),
            pl.BlockSpec((rows, 1), whole),
        ],
        out_shape=[
            jax.ShapeDtypeStruct((16, depth, LANES), BF),
            pltpu.HBM((rows, 2 * ff), BF),
            jax.ShapeDtypeStruct((rows, 1), F32),
        ],
        scratch_shapes=[
            pltpu.VMEM((rows, width), BF),
            pltpu.VMEM((rows, ff), BF),
            pltpu.VMEM((rows, 2 * ff), BF),
            pltpu.SemaphoreType.DMA,
        ],
        compiler_params=pltpu.CompilerParams(vmem_limit_bytes=36 * 2**20),
        cost_estimate=pl.CostEstimate(
            flops=16 * rows * width * ff, bytes_accessed=40 * 2**20, transcendentals=rows * ff
        ),
        name="expert_grads",
    )(w_gu, w_gu, in_hbm(w_dn), in_hbm(x), in_hbm(dy), row_prob)


def unpack_kernel(in_ref, gu_ref, dn_ref):
    at = 0
    for ref in (gu_ref, dn_ref):
        r = ref.shape[0]
        for t in range(ref.shape[1] // LANES):
            ref[:, t * LANES : (t + 1) * LANES] = in_ref[at : at + r, :]
            at += r


def unpack(total, width, ff):
    return pl.pallas_call(
        unpack_kernel,
        out_shape=[
            jax.ShapeDtypeStruct((width // 16, 2 * ff), BF),
            jax.ShapeDtypeStruct((ff // 16, width), BF),
        ],
        compiler_params=pltpu.CompilerParams(vmem_limit_bytes=8 * 2**20),
        name="unpack",
    )(in_hbm(total))


def step(tokens, out_grad, z_weight, router_weight, expert_ids, gate_up_weight, down_weight):
    tok, width = tokens.shape
    routed = router_weight.shape[1]
    cap = tok // 2
    w_gu = gate_up_weight[0]
    w_dn = down_weight[0]
    ff = w_dn.shape[0]
    my_y = lax.axis_index("y")
    my_c = lax.axis_index("c")

    names = jnp.arange(routed, dtype=jnp.int32)[None, :]
    slots = jnp.arange(cap, dtype=F32)[None, :, None]
    before = (jnp.arange(tok)[:, None] < jnp.arange(tok)[None, :]).astype(BF)
    top = expert_ids.shape[1]
    id_row = expert_ids.T.astype(BF).reshape(1, top * tok)
    x0 = jnp.concatenate([tokens, jnp.pad(id_row, ((0, 7), (0, width - top * tok)))], axis=0)
    logits = jnp.dot(tokens, router_weight, preferred_element_type=F32)
    chosen = expert_ids[:, 0:1] == names
    for k in range(1, top):
        chosen = chosen | (expert_ids[:, k : k + 1] == names)
    expl = jnp.exp(logits)
    sel_exp = jnp.where(chosen, expl, 0.0)
    probs = jnp.where(chosen, sel_exp / jnp.sum(sel_exp, axis=1, keepdims=True), 0.0)
    log_total = jnp.log(jnp.sum(expl, axis=1, keepdims=True))
    mine = probs[:, :8].T
    high = mine.astype(BF)
    low = (mine - high.astype(F32)).astype(BF)
    prob_row = jnp.concatenate([high.reshape(1, 8 * tok), low.reshape(1, 8 * tok)], axis=1)
    g0 = jnp.concatenate([out_grad, jnp.pad(prob_row, ((0, 7), (0, width - 16 * tok)))], axis=0)

    x1, x3 = shift(x0, 1), shift(x0, -1)
    g1, g3 = shift(g0, 1), shift(g0, -1)
    x2 = spread(x1, x3)
    g2 = spread(g1, g3)
    x_parts, g_parts = [], []
    for part in (x0, x1, x3, x2):
        x_parts += [part, swap(part)]
    for part in (g0, g1, g3, g2):
        g_parts += [part, swap(part)]
    gray = lambda k: k ^ (k >> 1)
    place = [gray((my_y - s // 2) % 4) * 2 + (my_c ^ (s % 2)) for s in range(8)]
    origin = [((my_y - gray(k)) % 4) * 2 + (my_c ^ cc) for k in range(4) for cc in range(2)]

    me = my_y * 2 + my_c

    def choose(parts):
        named = jnp.stack([p[tok, : top * tok].reshape(top, tok) for p in parts])
        member = jnp.max(jnp.where(named == me.astype(BF), 1.0, 0.0), axis=1)
        rank = jnp.dot(member.astype(BF), before, preferred_element_type=F32)
        return (rank[:, None, :] == slots) & (member[:, None, :] > 0.0)

    def compact(take, parts):
        rows = [
            jnp.dot(take[j].astype(BF), p[:tok], preferred_element_type=F32).astype(BF)
            for j, p in enumerate(parts)
        ]
        return jnp.concatenate(rows, axis=0)

    take_a = choose(x_parts[:6])
    xa = compact(take_a, x_parts[:6])
    take_b = choose(x_parts[6:])
    xb = compact(take_b, x_parts[6:])
    x = jnp.concatenate([xa, xb], axis=0)
    take = jnp.concatenate([take_a, take_b], axis=0)
    pick = (jnp.arange(16, dtype=jnp.int32) % 8 == me)[None, :, None]
    pairs = jnp.stack([p[tok, : 16 * tok].reshape(16, tok) for p in g_parts]).astype(F32)
    prob_of = jnp.sum(jnp.where(pick, pairs, 0.0), axis=1)
    row_prob = jnp.sum(jnp.where(take, prob_of[:, None, :], 0.0), axis=2).reshape(8 * cap, 1)
    dy = compact(take, g_parts)
    parts, pre, score = expert_grads(w_gu, w_dn, x, dy, row_prob)
    total = lax.psum_scatter(parts.reshape(1, -1, parts.shape[2]), DP, scatter_dimension=1, tiled=True)[0]
    gate_up_grad, down_grad = unpack(total, width, ff)

    home_score = send_each(jnp.concatenate(
        [lax.dynamic_slice_in_dim(score.reshape(8, 1, cap), s, 1, 0) for s in place], axis=0))
    row_grad = dot_t(pre, w_gu).astype(BF)
    row_grad = row_grad.reshape(8, cap, width)
    home_rows = send_each(jnp.concatenate(
        [lax.dynamic_slice_in_dim(row_grad, s, 1, 0) for s in place], axis=0))

    member = jnp.where(chosen[:, :8], 1.0, 0.0).T
    rank = jnp.dot(member.astype(BF), before, preferred_element_type=F32)
    back = (rank[:, None, :] == slots) & (member[:, None, :] > 0.0)
    score_of = jnp.sum(jnp.where(back, home_score.reshape(8, cap, 1), 0.0), axis=1)
    scores = jnp.concatenate([score_of.T, jnp.zeros((tok, routed - 8), F32)], axis=1)
    mean_score = jnp.sum(probs * scores, axis=1, keepdims=True)
    z_grad = 2.0 * z_weight[:, None] * log_total * jnp.exp(logits - log_total)
    logit_grad = (z_grad + probs * (scores - mean_score)).astype(BF)
    share = send_each(logit_grad.T.reshape(8, routed // 8, tok))
    share = jnp.concatenate([lax.dynamic_slice_in_dim(share, o, 1, 0)[0] for o in origin], axis=1)
    group_tokens = jnp.concatenate([p[:tok] for p in x_parts], axis=0)
    router_part = jnp.dot(share, group_tokens, preferred_element_type=F32)
    router_part = ring_all(ring_all(router_part, "x"), "z")
    near = lax.all_gather(router_part, "y", axis=0, tiled=False)
    away = swap(near)
    both = jnp.stack([jnp.where(my_c == 0, near, away), jnp.where(my_c == 0, away, near)], axis=1)
    router_grad = both.reshape(routed, width).T
    token_grad = (
        tdot(back.astype(BF).reshape(8 * cap, tok), home_rows.reshape(8 * cap, width))
        + dot_t(logit_grad, router_weight)
    ).astype(BF)
    return token_grad, router_grad, gate_up_grad[None], down_grad[None]


def solution(mesh):
    grid = Mesh(mesh.devices.reshape(4, 4, 4, 2), ("x", "z", "y", "c"))
    every = ("x", "z", "y", "c")
    return jax.shard_map(
        step,
        mesh=grid,
        in_specs=(
            P(every, None),
            P(every, None),
            P(every),
            P(),
            P(every, None),
            P(GROUP, None, None),
            P(GROUP, None, None),
        ),
        out_specs=(
            P(every, None),
            P(),
            P(GROUP, DP, None),
            P(GROUP, DP, None),
        ),
        check_vma=False,
    )
```
